256 devices in a mesh: tm: 32 (over y, z), chan: 8 (over x, core).
Axes of the slice: x: 4, y: 4, z: 8, core: 2. Of those that a mesh axis runs over, the one named last changes fastest.
Arguments:
- record: bfloat16 [114688, 10240], P('tm', 'chan'), may hold values from -256 to 256
- pilot_sweep: bfloat16 [3072], replicated, may hold values from -0.109375 to 0.109375
- sweep_table: int32 [3, 32], replicated, may hold values from 0 to 114687, as said below
- owner_map: int32 [8], replicated, may hold values from 0 to 7, each once
Outputs:
- stacks: float32 [8, 1024, 10240], P(None, 'tm', 'chan')
The draws below stay inside these ranges and needn't reach their ends.
Inputs may be any that keep to these rules, and one draw needn't show every extreme that they name: `sweep_table`: column g is sweep g: row 0 lies in [3584 g, 3584 g + 512]; row 1 is its shot, and every shot has at least one sweep; row 2 is the number of earlier sweeps with the same shot.
All inputs are finite; a program needn't handle non-finite values.
Results may differ from the reference program's by a relative error of at most 0.0029.
Values may be sent and summed in bfloat16 or wider, within the bound.
No kernel may reach another device: no remote copies, remote signals or barrier semaphores. Data moves between devices by JAX's collectives and lax.ppermute only.
A program may use at most 128 MiB of HBM per device.

```python
import jax
import jax.numpy as jnp
from jax import lax

CHANNELS = 10240
SWEEP = 3072
PILOT_SPACING = 3584
SEG = 1024
ITERS = 3
T_DEV = 3584
TRACE_LENGTH = 114688
SWEEPS = 32
SHOTS = 8
N_TM = 32
N_CHAN = 8


def draw_record(key, part):
    excitation_lines = PILOT_SPACING // 4
    excitation_segments = TRACE_LENGTH // excitation_lines
    position = jnp.arange(TRACE_LENGTH, dtype=jnp.float32) / TRACE_LENGTH
    channel_position = jnp.arange(CHANNELS, dtype=jnp.float32) / CHANNELS
    rough = jax.random.uniform(jax.random.fold_in(key, 3), (CHANNELS,), jnp.float32, 0.0, jnp.log(2.0))
    noise = jax.random.truncated_normal(jax.random.fold_in(key, 1), -4.0, 4.0, (TRACE_LENGTH, CHANNELS), jnp.float32)
    frequency_slope = jnp.exp(jnp.log(3.0) * position)
    single_excitation = jnp.exp(jax.random.uniform(jax.random.fold_in(key, 2), (excitation_segments,), jnp.float32, 0.0, jnp.log(2.0)))
    channel = jnp.exp(jnp.log(3.0) * channel_position + rough)
    cauchy_damping_factor = frequency_slope * jnp.repeat(single_excitation, excitation_lines)
    return (noise * cauchy_damping_factor[:, None] * channel[None, :]).astype(jnp.bfloat16)


def draw_sweep_table(key, part):
    count = SWEEPS
    order_index = jnp.arange(count, dtype=jnp.int32)
    jitter = jax.random.randint(jax.random.fold_in(key, 21), (count,), 0, PILOT_SPACING - SWEEP + 1)
    starts = order_index * PILOT_SPACING + jitter
    first = jax.random.randint(jax.random.fold_in(key, 22), (count,), 0, SHOTS)
    second = jax.random.randint(jax.random.fold_in(key, 23), (count,), 0, SHOTS)
    skewed = jnp.minimum(first, second)
    base = jnp.where(order_index < SHOTS, order_index, skewed)
    labels = base[jax.random.permutation(jax.random.fold_in(key, 24), count)]
    relabel = jax.random.permutation(jax.random.fold_in(key, 25), SHOTS).astype(jnp.int32)
    shots = relabel[labels]
    hits = (shots[:, None] == jnp.arange(SHOTS, dtype=jnp.int32)[None, :]).astype(jnp.int32)
    before = jnp.cumsum(hits, axis=0) - hits
    repeat_shot = jnp.sum(before * hits, axis=1)
    return jnp.stack([starts, shots, repeat_shot]).astype(jnp.int32)


def gaussian(key, dims, scale, bound, held_as=jnp.bfloat16):
    drawn = scale * jax.random.normal(key, dims, jnp.float32)
    return jnp.clip(drawn, min=-bound, max=bound).astype(held_as)


def setup_inputs(seed: int = 0) -> dict:
    key_list = jax.random.split(jax.random.key(seed), 5)
    return {
        "record": draw_record(jax.random.fold_in(key_list[4], 71), 0),
        "pilot_sweep": gaussian(key_list[1], (SWEEP,), SWEEP ** -0.5, 0.109375),
        "sweep_table": draw_sweep_table(jax.random.fold_in(key_list[4], 71), 0),
        "owner_map": jax.random.permutation(key_list[3], SHOTS).astype(jnp.int32),
    }


EPSILON = 1e-6


def reference(record, pilot_sweep, sweep_table, owner_map):
    block_width = CHANNELS // N_CHAN
    width = SEG + SWEEP
    lag_index = jnp.arange(width, dtype=jnp.int32)[None, :] - jnp.arange(SEG, dtype=jnp.int32)[:, None]
    inside = (lag_index >= 0) & (lag_index < SWEEP)
    tapped = pilot_sweep[jnp.clip(lag_index, 0, SWEEP - 1)]
    toeplitz = jnp.where(inside, tapped, jnp.zeros_like(tapped))
    polarity = 1.0 - 2.0 * (sweep_table[2] % 2).astype(jnp.float32)

    def one_sweep(index):
        block_start = index * T_DEV
        first = lax.dynamic_slice_in_dim(record, block_start, T_DEV, 0)
        following = lax.dynamic_slice_in_dim(record, jnp.minimum(index + 1, N_TM - 1) * T_DEV, T_DEV, 0)
        following = jnp.where(index + 1 < N_TM, following, jnp.zeros_like(following))
        joined = jnp.concatenate([first, following], axis=0)
        offset = (sweep_table[0, index] - block_start).astype(jnp.int32)
        window = lax.dynamic_slice_in_dim(joined, offset, width, 0)
        correlation = jnp.dot(toeplitz, window, preferred_element_type=jnp.float32)
        return (correlation * polarity[index]).astype(jnp.bfloat16)

    traces = lax.map(one_sweep, jnp.arange(SWEEPS, dtype=jnp.int32))
    trace_blocks = traces.reshape(SWEEPS, SEG, N_CHAN, block_width).transpose(2, 0, 1, 3)
    shot_of = sweep_table[1]
    member = (shot_of[:, None] == jnp.arange(SHOTS, dtype=jnp.int32)[None, :]).astype(jnp.float32)
    member_half = member.astype(jnp.bfloat16)
    counts = jnp.sum(member, axis=0)

    def first_stack(trace_block):
        summed = jnp.dot(member_half.T, trace_block.reshape(SWEEPS, SEG * block_width), preferred_element_type=jnp.float32)
        return summed.reshape(SHOTS, SEG, block_width) / counts[:, None, None]

    stack_blocks = lax.map(first_stack, trace_blocks)

    def energy_block(pair):
        trace_block, stack_block = pair
        fitted = stack_block[shot_of]
        return jnp.mean(jnp.square(trace_block.astype(jnp.float32) - fitted), axis=1)

    for iteration in range(ITERS):
        energies = lax.map(energy_block, (trace_blocks, stack_blocks))
        spread = jnp.sum(energies) / (SWEEPS * CHANNELS) + EPSILON

        def update_block(pair, spread=spread):
            trace_block, energy = pair
            weight = 1.0 / (1.0 + energy / spread)
            weighted = weight[:, None, :] * trace_block.astype(jnp.float32)
            numerator = jnp.einsum("gk,guc->kuc", member, weighted, precision=lax.Precision.HIGHEST)
            denominator = jnp.dot(member.T, weight, precision=lax.Precision.HIGHEST)
            return numerator / denominator[:, None, :]

        stack_blocks = lax.map(update_block, (trace_blocks, energies))
    stacked = stack_blocks.transpose(1, 2, 0, 3).reshape(SHOTS, SEG, CHANNELS)
    return jnp.zeros_like(stacked).at[owner_map].set(stacked)
```

```python
import functools

import jax
import jax.numpy as jnp
from jax import lax
from jax.experimental import pallas as pl
from jax.experimental.pallas import tpu as pltpu
from jax.sharding import PartitionSpec as P

SEG = 1024
ITERS = 3
EPSILON = 1e-06
BLOCK = 256
GROUP = 8
AXES = ("tm", "chan")
F32 = jnp.float32
BF16 = jnp.bfloat16


def toeplitz_block(pilot, offset, width):
    row = lax.dynamic_update_slice(jnp.zeros((width + 1,), pilot.dtype), pilot, (offset,))
    return jnp.tile(row, BLOCK)[: BLOCK * width].reshape(BLOCK, width)


def to_column(row):
    size = row.shape[1]
    eye = lax.broadcasted_iota(jnp.int32, (size, size), 0) == lax.broadcasted_iota(jnp.int32, (size, size), 1)
    return jnp.sum(jnp.where(eye, row, 0.0), axis=1, keepdims=True)


def residual_energy(gram, norm, same, weight):
    column = to_column(weight)
    cross = jnp.sum(gram * column, axis=0, keepdims=True)
    total = jnp.sum(same * column, axis=0, keepdims=True)
    square = jnp.sum(same * to_column(weight * cross), axis=0, keepdims=True)
    inverse = 1.0 / total
    energy = norm - 2.0 * cross * inverse + square * inverse * inverse
    return jnp.maximum(energy, 0.0) * (1.0 / SEG)


def group_rows(samples, i):
    part = samples[:, i * GROUP : (i + 1) * GROUP, :].astype(F32)
    return part.reshape(part.shape[0] * GROUP, part.shape[2]).astype(BF16)


def gram_kernel(samples, key_col, key_row, gram_out, norm_out, energy_out, total_out):
    same = (key_col[...] == key_row[...]).astype(F32)
    size = same.shape[0]
    eye = lax.broadcasted_iota(jnp.int32, (size, size), 0) == lax.broadcasted_iota(jnp.int32, (size, size), 1)
    total = jnp.zeros((1, size), F32)
    for i in range(gram_out.shape[0]):
        rows = group_rows(samples, i)
        product = lax.dot_general(rows, rows, (((1,), (1,)), ((), ())), preferred_element_type=F32)
        norm = jnp.sum(jnp.where(eye, product, 0.0), axis=0, keepdims=True)
        gram = product * same
        energy = residual_energy(gram, norm, same, jnp.ones((1, size), F32))
        gram_out[i] = gram
        norm_out[i] = norm
        energy_out[i] = energy
        total = total + energy
    total_out[...] = jnp.broadcast_to(jnp.sum(total, axis=1, keepdims=True), total_out.shape)


def spread_of(arrived, scale):
    return jnp.sum(arrived[...], axis=0)[:, :1] * scale + EPSILON


def update_kernel(scale, arrived, gram_in, norm_in, energy_in, key_col, key_row, energy_out, total_out):
    same = (key_col[...] == key_row[...]).astype(F32)
    spread = spread_of(arrived, scale)
    total = jnp.zeros((1, same.shape[0]), F32)
    for i in range(gram_in.shape[0]):
        weight = 1.0 / (1.0 + energy_in[i] / spread)
        energy = residual_energy(gram_in[i], norm_in[i], same, weight)
        energy_out[i] = energy
        total = total + energy
    total_out[...] = jnp.broadcast_to(jnp.sum(total, axis=1, keepdims=True), total_out.shape)


def stack_kernel(scale, arrived, samples, energy_in, key_col, key_row, out):
    same = (key_col[...] == key_row[...]).astype(F32)
    spread = spread_of(arrived, scale)
    shots = 8
    slots = lax.broadcasted_iota(jnp.int32, (shots * GROUP, same.shape[0]), 0)
    mine = slots == key_row[...]
    span = out.shape[2] // shots
    per_tile = 128 // span
    lane = lax.broadcasted_iota(jnp.int32, (GROUP, 128), 1) // span
    for i in range(energy_in.shape[0]):
        rows = group_rows(samples, i)
        weight = 1.0 / (1.0 + energy_in[i] / spread)
        total = jnp.sum(same * to_column(weight), axis=0, keepdims=True)
        factor = jnp.where(mine, weight / total, 0.0)
        high = factor.astype(BF16)
        rest = factor - high.astype(F32)
        middle = rest.astype(BF16)
        low = (rest - middle.astype(F32)).astype(BF16)
        stack = jnp.dot(high, rows, preferred_element_type=F32)
        stack = stack + jnp.dot(middle, rows, preferred_element_type=F32)
        stack = stack + jnp.dot(low, rows, preferred_element_type=F32)
        for tile in range(stack.shape[1] // 128):
            for half in range(shots // per_tile):
                pieces = []
                for p in range(per_tile):
                    k = half * per_tile + p
                    pieces.append(stack[k * GROUP : (k + 1) * GROUP, tile * 128 : (tile + 1) * 128])
                for d in range(per_tile):
                    merged = None
                    for p in range(per_tile):
                        moved = pieces[p] if p == d else pltpu.roll(pieces[p], (span * (p - d)) % 128, 1)
                        merged = moved if merged is None else jnp.where(lane == p, moved, merged)
                    out[tile * per_tile + d, i * GROUP : (i + 1) * GROUP, half * 128 : (half + 1) * 128] = merged.astype(
                        out.dtype
                    )


VMEM = pl.BlockSpec(memory_space=pltpu.VMEM)


def shards(record, pilot_sweep, sweep_table, owner_map):
    block_rows, channels = record.shape
    devices = lax.axis_size("tm")
    own = channels // devices
    following = lax.ppermute(record[:SEG], "tm", [(k, k - 1) for k in range(1, devices)])
    here = lax.axis_index("tm")
    column = lax.dynamic_slice_in_dim(sweep_table, here, 1, 1)[:, 0]
    offset = column[0] - here * block_rows
    taps = toeplitz_block(pilot_sweep, offset, block_rows + BLOCK)
    contract = (((0,), (1,)), ((), ()))
    polarity = 1.0 - 2.0 * (column[2] % 2).astype(F32)
    blocks = []
    for b in range(SEG // BLOCK):
        split = block_rows - BLOCK * b
        near = lax.dot_general(record[BLOCK * b :], taps[:, :split], contract, preferred_element_type=F32)
        far = lax.dot_general(following[: BLOCK * (b + 1)], taps[:, split:], contract, preferred_element_type=F32)
        blocks.append(((near + far) * polarity).astype(BF16))
    traces = jnp.concatenate(blocks, axis=1).reshape(devices, own, SEG)
    slot = owner_map[sweep_table[1]]
    key = (slot[:, None] * GROUP + jnp.arange(GROUP, dtype=jnp.int32)[None, :]).reshape(-1)
    traces, key_col, key_row = lax.optimization_barrier((traces, key[:, None], key[None, :]))
    samples = lax.all_to_all(traces, "tm", 0, 0, tiled=True)

    groups = own // GROUP
    size = key.shape[0]
    wide = lax.axis_size("chan")
    gram_shape = jax.ShapeDtypeStruct((groups, size, size), F32)
    row_shape = jax.ShapeDtypeStruct((groups, 1, size), F32)
    one = jax.ShapeDtypeStruct((wide, 1, 128), F32)
    scale = 1.0 / (devices * channels * wide)

    def exchanged(total):
        row = lax.all_to_all(total, "chan", 0, 0, tiled=True).sum(axis=0)
        return lax.all_to_all(jnp.broadcast_to(row[None], (devices, *row.shape)), "tm", 0, 0, tiled=True)

    gram, norm, energy, total = pl.pallas_call(
        gram_kernel, out_shape=(gram_shape, row_shape, row_shape, one), in_specs=[VMEM] * 3, out_specs=(VMEM,) * 4, name="gram"
    )(samples, key_col, key_row)
    for _ in range(ITERS - 1):
        energy, total = pl.pallas_call(
            functools.partial(update_kernel, scale), out_shape=(row_shape, one), in_specs=[VMEM] * 6, out_specs=(VMEM,) * 2, name="update"
        )(exchanged(total), gram, norm, energy, key_col, key_row)
    shots = owner_map.shape[0]
    span = SEG // devices
    parts = pl.pallas_call(
        functools.partial(stack_kernel, scale),
        out_shape=jax.ShapeDtypeStruct((devices, own, shots * span), BF16),
        in_specs=[VMEM] * 5,
        out_specs=VMEM,
        name="stack",
    )(exchanged(total), samples, energy, key_col, key_row)
    arrived = lax.all_to_all(parts, "tm", 0, 0, tiled=True)
    return arrived.reshape(channels, shots * span).T.astype(F32).reshape(shots, span, channels)


def solution(mesh):
    placed = (P("tm", "chan"), P(), P(), P())
    return jax.shard_map(
        shards, mesh=mesh, in_specs=placed, out_specs=P(None, "tm", "chan"), check_vma=False
    )
```

```python
import functools

import jax
import jax.numpy as jnp
from jax import lax
from jax.experimental import pallas as pl
from jax.experimental.pallas import tpu as pltpu
from jax.sharding import PartitionSpec as P

SEG = 1024
ITERS = 3
EPSILON = 1e-06
BLOCK = 256
GROUP = 8
STEP = 16
AHEAD = 256
TILE = 256
F32 = jnp.float32
BF16 = jnp.bfloat16


def shifted_rows(row, out):
    base = pltpu.roll(jnp.broadcast_to(row, (STEP, row.shape[1])), 0, 1, stride=1, stride_axis=0)
    skip = row.shape[1] - out.shape[1]
    for k in range(BLOCK // STEP):
        moved = base if k == 0 else pltpu.roll(base, STEP * k, 1)
        out[k * STEP : (k + 1) * STEP, :] = moved[:, skip:].astype(out.dtype)


def toeplitz_kernel(block_rows, here, table, pilot, taps, taps_before):
    at = here[0]
    before = jnp.where(at == 0, table.shape[1] - 1, at - 1)
    skip = pilot.shape[1] - taps_before.shape[1] - BLOCK
    shifted_rows(pltpu.roll(pilot[...], table[0, at] - at * block_rows, 1), taps)
    moved = pltpu.roll(pilot[...], table[0, before] - before * block_rows, 1)[:, skip:]
    shifted_rows(jnp.where(at == 0, 0.0, moved), taps_before)


def sign_of(table, column):
    return 1.0 - 2.0 * (table[2, column] % 2).astype(F32)


def transposed_into(out, first, block, values, sign):
    rounded = (values * sign).astype(BF16)
    for k in range(values.shape[1] // 128):
        out[first + 128 * k : first + 128 * (k + 1), block * BLOCK : (block + 1) * BLOCK] = rounded[:, 128 * k : 128 * (k + 1)].T


def side_kernel(taps, taps_before, record, near_out, behind_out):
    rows = record.shape[0]
    for b in range(near_out.shape[0]):
        product = jnp.dot(taps[:, : rows - BLOCK * b], record[BLOCK * b :, :], preferred_element_type=F32)
        near_out[b] = product
    for b in range(near_out.shape[0]):
        kept = taps_before.shape[1] - BLOCK * (b + 1)
        behind_out[b] = jnp.dot(taps_before[:, kept:], record[: BLOCK * (b + 1), :], preferred_element_type=F32)


def near_kernel(taps, record, near_out):
    rows = record.shape[0]
    for b in range(near_out.shape[0]):
        product = jnp.dot(taps[:, : rows - BLOCK * b], record[BLOCK * b :, :], preferred_element_type=F32)
        near_out[b] = product


def far_kernel(here, table, taps, near, following, early_out, last_out):
    sign = sign_of(table, here[0])
    count = near.shape[0]
    for b in range(count):
        rows = min(BLOCK * (b + 1), following.shape[0])
        split = taps.shape[1] - BLOCK * (b + 1)
        values = near[b] + jnp.dot(taps[:, split : split + rows], following[:rows, :], preferred_element_type=F32)
        if b < count - 1:
            transposed_into(early_out, 0, b, values, sign)
        else:
            last_out[...] = values


def late_kernel(here, table, taps_last, last, rest, ahead, behind, early, out):
    at = here[0]
    before = jnp.where(at == 0, table.shape[1] - 1, at - 1)
    count = ahead.shape[0]
    first = ahead.shape[2]
    out[first:, : early.shape[1]] = early[...]
    for b in range(count):
        transposed_into(out, 0, b, ahead[b] + behind[b], sign_of(table, before))
    product = jnp.dot(taps_last[...], rest[...], preferred_element_type=F32)
    transposed_into(out, first, count - 1, last[...] + product, sign_of(table, at))


def to_column(row):
    size = row.shape[1]
    eye = lax.broadcasted_iota(jnp.int32, (size, size), 0) == lax.broadcasted_iota(jnp.int32, (size, size), 1)
    return jnp.sum(jnp.where(eye, row, 0.0), axis=1, keepdims=True)


def residual_energy(gram, norm, same, weight):
    column = to_column(weight)
    cross = jnp.sum(gram * column, axis=0, keepdims=True)
    total = jnp.sum(same * column, axis=0, keepdims=True)
    square = jnp.sum(same * to_column(weight * cross), axis=0, keepdims=True)
    inverse = 1.0 / total
    energy = norm - 2.0 * cross * inverse + square * inverse * inverse
    return jnp.maximum(energy, 0.0) * (1.0 / SEG)


def group_rows(samples, i):
    part = samples[:, i * GROUP : (i + 1) * GROUP, :].astype(F32)
    return part.reshape(part.shape[0] * GROUP, part.shape[2]).astype(BF16)


def same_shot(key):
    return (to_column(key) == key).astype(F32)


def gram_kernel(here, table, owner, samples, keys, gram_out, norm_out, energy_out, total_out):
    size = keys.shape[2]
    eye = lax.broadcasted_iota(jnp.int32, (size, size), 0) == lax.broadcasted_iota(jnp.int32, (size, size), 1)
    total = jnp.zeros((1, size), F32)
    lane = lax.broadcasted_iota(jnp.int32, (1, size), 1)
    sweeps = table.shape[1]
    usual = jnp.zeros((1, size), F32)
    moved = jnp.zeros((1, size), F32)
    for g in range(sweeps):
        slot = owner[table[1, g]].astype(F32) * GROUP
        usual = jnp.where(lane // GROUP == g, slot, usual)
        moved = jnp.where(lane // GROUP == (g + 1) % sweeps, slot, moved)
    offset = (lane % GROUP).astype(F32)
    own = gram_out.shape[0] * GROUP
    for i in range(gram_out.shape[0]):
        key = jnp.where(here[0] * own + i * GROUP < AHEAD, moved, usual) + offset
        keys[i] = key
        same = same_shot(key)
        rows = group_rows(samples, i)
        product = lax.dot_general(rows, rows, (((1,), (1,)), ((), ())), preferred_element_type=F32)
        norm = jnp.sum(jnp.where(eye, product, 0.0), axis=0, keepdims=True)
        gram = product * same
        energy = residual_energy(gram, norm, same, jnp.ones((1, size), F32))
        gram_out[i] = gram
        norm_out[i] = norm
        energy_out[i] = energy
        total = total + energy
    total_out[...] = jnp.broadcast_to(jnp.sum(total, axis=1, keepdims=True), total_out.shape)


def spread_of(arrived, scale):
    return jnp.sum(arrived[...], axis=0)[:, :1] * scale + EPSILON


def update_kernel(scale, arrived, gram_in, norm_in, energy_in, keys, energy_out, total_out):
    spread = spread_of(arrived, scale)
    total = jnp.zeros((1, keys.shape[2]), F32)
    for i in range(gram_in.shape[0]):
        weight = 1.0 / (1.0 + energy_in[i] / spread)
        energy = residual_energy(gram_in[i], norm_in[i], same_shot(keys[i]), weight)
        energy_out[i] = energy
        total = total + energy
    total_out[...] = jnp.broadcast_to(jnp.sum(total, axis=1, keepdims=True), total_out.shape)


def stack_kernel(scale, arrived, samples, energy_in, keys, out):
    spread = spread_of(arrived, scale)
    shots = 8
    slots = lax.broadcasted_iota(jnp.int32, (shots * GROUP, keys.shape[2]), 0).astype(F32)
    span = out.shape[2] // shots
    per_tile = 128 // span
    lane = lax.broadcasted_iota(jnp.int32, (GROUP, 128), 1) // span
    for i in range(energy_in.shape[0]):
        rows = group_rows(samples, i)
        weight = 1.0 / (1.0 + energy_in[i] / spread)
        total = jnp.sum(same_shot(keys[i]) * to_column(weight), axis=0, keepdims=True)
        factor = jnp.where(slots == keys[i], weight / total, 0.0)
        high = factor.astype(BF16)
        rest = factor - high.astype(F32)
        middle = rest.astype(BF16)
        low = (rest - middle.astype(F32)).astype(BF16)
        stack = jnp.dot(high, rows, preferred_element_type=F32)
        stack = stack + jnp.dot(middle, rows, preferred_element_type=F32)
        stack = stack + jnp.dot(low, rows, preferred_element_type=F32)
        for tile in range(stack.shape[1] // 128):
            for half in range(shots // per_tile):
                pieces = []
                for p in range(per_tile):
                    k = half * per_tile + p
                    pieces.append(stack[k * GROUP : (k + 1) * GROUP, tile * 128 : (tile + 1) * 128])
                for d in range(per_tile):
                    merged = None
                    for p in range(per_tile):
                        moved = pieces[p] if p == d else pltpu.roll(pieces[p], (span * (p - d)) % 128, 1)
                        merged = moved if merged is None else jnp.where(lane == p, moved, merged)
                    out[tile * per_tile + d, i * GROUP : (i + 1) * GROUP, half * 128 : (half + 1) * 128] = merged.astype(
                        out.dtype
                    )


VMEM = pl.BlockSpec(memory_space=pltpu.VMEM)
SMEM = pl.BlockSpec(memory_space=pltpu.SMEM)


def shards(record, pilot_sweep, sweep_table, owner_map):
    block_rows, channels = record.shape
    devices = lax.axis_size("tm")
    own = channels // devices
    blocks = SEG // BLOCK
    here = lax.axis_index("tm")
    width = block_rows + BLOCK
    kept = SEG - BLOCK
    back = [(k, k - 1) for k in range(1, devices)]
    forth = [(k, (k + 1) % devices) for k in range(devices)]
    first_rows = lax.ppermute(record[:kept, AHEAD:], "tm", back)
    last_rows = lax.ppermute(record[kept:SEG, AHEAD:], "tm", back)
    at = here.astype(jnp.int32).reshape(1)
    shape = jax.ShapeDtypeStruct
    pilot = jnp.pad(pilot_sweep.astype(F32), (0, width - pilot_sweep.shape[0]))[None]
    taps, taps_before = pl.pallas_call(
        functools.partial(toeplitz_kernel, block_rows),
        out_shape=(shape((BLOCK, width), BF16), shape((BLOCK, SEG), BF16)),
        in_specs=[SMEM, SMEM, VMEM],
        out_specs=(VMEM,) * 2,
        name="toeplitz",
    )(at, sweep_table, pilot)
    piece = shape((blocks, BLOCK, AHEAD), F32)
    near, behind = pl.pallas_call(
        side_kernel,
        grid=(1,),
        out_shape=(piece, piece),
        in_specs=[
            pl.BlockSpec((BLOCK, width), lambda i: (0, 0)),
            pl.BlockSpec((BLOCK, SEG), lambda i: (0, 0)),
            pl.BlockSpec((block_rows, AHEAD), lambda i: (0, 0)),
        ],
        out_specs=(pl.BlockSpec((blocks, BLOCK, AHEAD), lambda i: (0, 0, 0)),) * 2,
        name="side",
    )(taps, taps_before, record)
    ahead = lax.ppermute(near, "tm", forth)
    others = channels - AHEAD
    near = pl.pallas_call(
        near_kernel,
        grid=(others // TILE,),
        out_shape=shape((blocks, BLOCK, others), F32),
        in_specs=[
            pl.BlockSpec((BLOCK, width), lambda i: (0, 0)),
            pl.BlockSpec((block_rows, TILE), lambda i: (0, i + AHEAD // TILE)),
        ],
        out_specs=pl.BlockSpec((blocks, BLOCK, TILE), lambda i: (0, 0, i)),
        name="near",
    )(taps, record)
    early, last = pl.pallas_call(
        far_kernel,
        grid=(others // TILE,),
        out_shape=(shape((others, kept), BF16), shape((BLOCK, others), F32)),
        in_specs=[
            SMEM,
            SMEM,
            pl.BlockSpec((BLOCK, width), lambda i: (0, 0)),
            pl.BlockSpec((blocks, BLOCK, TILE), lambda i: (0, 0, i)),
            pl.BlockSpec((kept, TILE), lambda i: (0, i)),
        ],
        out_specs=(pl.BlockSpec((TILE, kept), lambda i: (i, 0)), pl.BlockSpec((BLOCK, TILE), lambda i: (0, i))),
        name="far",
    )(at, sweep_table, taps, near, first_rows)
    traces = pl.pallas_call(
        late_kernel,
        out_shape=shape((channels, SEG), BF16),
        in_specs=[SMEM] * 2 + [VMEM] * 6,
        out_specs=VMEM,
        name="late",
    )(at, sweep_table, taps[:, block_rows:], last, last_rows, ahead, behind, early)
    samples = lax.all_to_all(traces.reshape(devices, own, SEG), "tm", 0, 0, tiled=True)

    groups = own // GROUP
    size = sweep_table.shape[1] * GROUP
    wide = lax.axis_size("chan")
    gram_shape = jax.ShapeDtypeStruct((groups, size, size), F32)
    row_shape = jax.ShapeDtypeStruct((groups, 1, size), F32)
    one = jax.ShapeDtypeStruct((wide, 1, 128), F32)
    scale = 1.0 / (devices * channels * wide)

    def exchanged(total):
        row = lax.all_to_all(total, "chan", 0, 0, tiled=True).sum(axis=0)
        return lax.all_to_all(jnp.broadcast_to(row[None], (devices, *row.shape)), "tm", 0, 0, tiled=True)

    keys, gram, norm, energy, total = pl.pallas_call(
        gram_kernel,
        out_shape=(row_shape, gram_shape, row_shape, row_shape, one),
        in_specs=[SMEM] * 3 + [VMEM],
        out_specs=(VMEM,) * 5,
        name="gram",
    )(at, sweep_table, owner_map, samples)
    for _ in range(ITERS - 1):
        energy, total = pl.pallas_call(
            functools.partial(update_kernel, scale), out_shape=(row_shape, one), in_specs=[VMEM] * 5, out_specs=(VMEM,) * 2, name="update"
        )(exchanged(total), gram, norm, energy, keys)
    shots = owner_map.shape[0]
    span = SEG // devices
    parts = pl.pallas_call(
        functools.partial(stack_kernel, scale),
        out_shape=jax.ShapeDtypeStruct((devices, own, shots * span), BF16),
        in_specs=[VMEM] * 4,
        out_specs=VMEM,
        name="stack",
    )(exchanged(total), samples, energy, keys)
    arrived = lax.all_to_all(parts, "tm", 0, 0, tiled=True)
    return arrived.reshape(channels, shots * span).T.astype(F32).reshape(shots, span, channels)


def solution(mesh):
    placed = (P("tm", "chan"), P(), P(), P())
    return jax.shard_map(
        shards, mesh=mesh, in_specs=placed, out_specs=P(None, "tm", "chan"), check_vma=False
    )
```

```python
import functools

import jax
import jax.numpy as jnp
from jax import lax
from jax.experimental import pallas as pl
from jax.experimental.pallas import tpu as pltpu
from jax.sharding import PartitionSpec as P

SEG = 1024
ITERS = 3
EPSILON = 1e-06
BLOCK = 256
GROUP = 8
STEP = 16
AHEAD = 256
TILE = 256
F32 = jnp.float32
BF16 = jnp.bfloat16


def shifted_rows(row, out):
    base = pltpu.roll(jnp.broadcast_to(row, (STEP, row.shape[1])), 0, 1, stride=1, stride_axis=0)
    skip = row.shape[1] - out.shape[1]
    for k in range(BLOCK // STEP):
        moved = base if k == 0 else pltpu.roll(base, STEP * k, 1)
        out[k * STEP : (k + 1) * STEP, :] = moved[:, skip:].astype(out.dtype)


def toeplitz_kernel(block_rows, here, table, pilot, taps, taps_before, taps_last):
    at = here[0]
    before = jnp.where(at == 0, table.shape[1] - 1, at - 1)
    skip = pilot.shape[1] - taps_before.shape[1] - BLOCK
    shifted_rows(pltpu.roll(pilot[...], table[0, at] - at * block_rows, 1), taps)
    moved = pltpu.roll(pilot[...], table[0, before] - before * block_rows, 1)[:, skip:]
    shifted_rows(jnp.where(at == 0, 0.0, moved), taps_before)
    taps_last[...] = taps[:, block_rows:]


def sign_of(table, column):
    return 1.0 - 2.0 * (table[2, column] % 2).astype(F32)


def transposed_into(out, first, block, values, sign):
    rounded = (values * sign).astype(BF16)
    for k in range(values.shape[1] // 128):
        out[first + 128 * k : first + 128 * (k + 1), block * BLOCK : (block + 1) * BLOCK] = rounded[:, 128 * k : 128 * (k + 1)].T


def side_kernel(taps, taps_before, record, near_out, behind_out):
    rows = record.shape[0]
    for b in range(near_out.shape[0]):
        product = jnp.dot(taps[:, : rows - BLOCK * b], record[BLOCK * b :, :], preferred_element_type=F32)
        near_out[b] = product
    for b in range(near_out.shape[0]):
        kept = taps_before.shape[1] - BLOCK * (b + 1)
        behind_out[b] = jnp.dot(taps_before[:, kept:], record[: BLOCK * (b + 1), :], preferred_element_type=F32)


def near_kernel(taps, record, near_out):
    rows = record.shape[0]
    for b in range(near_out.shape[0]):
        product = jnp.dot(taps[:, : rows - BLOCK * b], record[BLOCK * b :, :], preferred_element_type=F32)
        near_out[b] = product


def far_kernel(here, table, taps, near, following, early_out, last_out):
    sign = sign_of(table, here[0])
    count = near.shape[0]
    for t in range(near.shape[2] // TILE):
        part = slice(TILE * t, TILE * (t + 1))
        for b in range(count):
            rows = min(BLOCK * (b + 1), following.shape[0])
            split = taps.shape[1] - BLOCK * (b + 1)
            product = jnp.dot(taps[:, split : split + rows], following[:rows, part], preferred_element_type=F32)
            values = near[b, :, part] + product
            if b < count - 1:
                transposed_into(early_out, TILE * t, b, values, sign)
            else:
                last_out[:, part] = values


def late_kernel(here, table, taps_last, last, rest, ahead, behind, early, out):
    at = here[0]
    before = jnp.where(at == 0, table.shape[1] - 1, at - 1)
    count = ahead.shape[0]
    first = ahead.shape[2]
    out[first:, : early.shape[1]] = early[...]
    for b in range(count):
        transposed_into(out, 0, b, ahead[b] + behind[b], sign_of(table, before))
    product = jnp.dot(taps_last[...], rest[...], preferred_element_type=F32)
    transposed_into(out, first, count - 1, last[...] + product, sign_of(table, at))


def lane_sum(values):
    row = values[:, :128] + values[:, 128:]
    step = GROUP
    while step < 128:
        row = row + pltpu.roll(row, step, 1)
        step *= 2
    return row


def twice(values):
    return jnp.concatenate([values, values], axis=1)


def down(values):
    return jnp.sum(values, axis=0, keepdims=True)


def combined(norm, cross, total, square):
    inverse = 1.0 / total
    energy = norm - 2.0 * cross * inverse + square * inverse * inverse
    return jnp.maximum(energy, 0.0) * (1.0 / SEG)


def residual_energy(gram, same, norm_side, norm_row, side, row):
    wide = twice(side)
    cross_side = lane_sum(gram * row)
    cross_row = down(gram * wide)
    total_side = lane_sum(same * row)
    total_row = down(same * wide)
    square_side = lane_sum(same * (row * cross_row))
    square_row = down(same * twice(side * cross_side))
    return combined(norm_side, cross_side, total_side, square_side), combined(norm_row, cross_row, total_row, square_row)


def group_rows(samples, i):
    part = samples[:, i * GROUP : (i + 1) * GROUP, :].astype(F32)
    return part.reshape(part.shape[0] * GROUP, part.shape[2]).astype(BF16)


def gram_kernel(here, table, owner, samples, keys, same_out, gram_out, norm_side, norm_row, energy_side, energy_row, total_out):
    groups = gram_out.shape[0]
    sweeps = table.shape[1]
    size = sweeps * GROUP
    lane = lax.broadcasted_iota(jnp.int32, (1, size), 1)
    line = lax.broadcasted_iota(jnp.int32, (sweeps, 1), 0)
    usual_row = moved_row = jnp.zeros((1, size), jnp.int32)
    usual_side = moved_side = jnp.zeros((sweeps, 1), jnp.int32)
    for g in range(sweeps):
        slot = owner[table[1, g]]
        after = (g + 1) % sweeps
        usual_row = jnp.where(lane // GROUP == g, slot, usual_row)
        usual_side = jnp.where(line == g, slot, usual_side)
        moved_row = jnp.where(lane // GROUP == after, slot, moved_row)
        moved_side = jnp.where(line == after, slot, moved_side)
    matching = lax.broadcasted_iota(jnp.int32, (GROUP, size), 0) == lane % GROUP
    ones = jnp.ones((sweeps, 128), F32)
    total = jnp.zeros((1, size), F32)
    for i in range(groups):
        ahead = (here[0] * groups + i) * GROUP < AHEAD
        row = jnp.where(ahead, moved_row, usual_row)
        side = jnp.where(ahead, moved_side, usual_side)
        keys[i] = (row * GROUP + lane % GROUP).astype(F32)
        same = (side == row).astype(F32)
        rows = group_rows(samples, i)
        product = lax.dot_general(rows, rows, (((1,), (1,)), ((), ())), preferred_element_type=F32)
        parts = product.reshape(sweeps, GROUP, size)
        full = jnp.sum(jnp.where(matching[None], parts, 0.0), axis=1)
        own = jnp.where(line == lane // GROUP, full, 0.0)
        gram = full * same
        norms = (lane_sum(own), down(own))
        same_out[i] = same
        gram_out[i] = gram
        norm_side[i], norm_row[i] = norms
        energy_side[i], energy = residual_energy(gram, same, *norms, ones, jnp.ones((1, size), F32))
        energy_row[i] = energy
        total = total + energy
    total_out[...] = jnp.broadcast_to(jnp.sum(total, axis=1, keepdims=True), total_out.shape)


def spread_of(arrived, scale):
    return jnp.sum(arrived[...], axis=0)[:, :1] * scale + EPSILON


def update_kernel(scale, arrived, same, gram, norm_side, norm_row, side_in, row_in, energy_side, energy_row, total_out):
    spread = spread_of(arrived, scale)
    total = jnp.zeros(row_in.shape[1:], F32)
    for i in range(gram.shape[0]):
        side = 1.0 / (1.0 + side_in[i] / spread)
        row = 1.0 / (1.0 + row_in[i] / spread)
        energy_side[i], energy = residual_energy(gram[i], same[i], norm_side[i], norm_row[i], side, row)
        energy_row[i] = energy
        total = total + energy
    total_out[...] = jnp.broadcast_to(jnp.sum(total, axis=1, keepdims=True), total_out.shape)


def stack_kernel(scale, shots, arrived, samples, keys, same, side_in, row_in, out):
    spread = spread_of(arrived, scale)
    size = keys.shape[2]
    slots = lax.broadcasted_iota(jnp.int32, (shots * GROUP, size), 0).astype(F32)
    span = out.shape[2] // shots
    per_tile = 128 // span
    lane = lax.broadcasted_iota(jnp.int32, (GROUP, 128), 1) // span
    for i in range(keys.shape[0]):
        rows = group_rows(samples, i)
        side = 1.0 / (1.0 + side_in[i] / spread)
        row = 1.0 / (1.0 + row_in[i] / spread)
        factor = jnp.where(slots == keys[i], row / down(same[i] * twice(side)), 0.0)
        high = factor.astype(BF16)
        rest = factor - high.astype(F32)
        middle = rest.astype(BF16)
        low = (rest - middle.astype(F32)).astype(BF16)
        products = jnp.dot(jnp.concatenate([high, middle, low], axis=0), rows, preferred_element_type=F32)
        count = shots * GROUP
        stack = products[:count] + products[count : 2 * count] + products[2 * count :]
        for tile in range(stack.shape[1] // 128):
            for half in range(shots // per_tile):
                pieces = []
                for p in range(per_tile):
                    k = half * per_tile + p
                    pieces.append(stack[k * GROUP : (k + 1) * GROUP, tile * 128 : (tile + 1) * 128])
                for d in range(per_tile):
                    merged = None
                    for p in range(per_tile):
                        moved = pieces[p] if p == d else pltpu.roll(pieces[p], (span * (p - d)) % 128, 1)
                        merged = moved if merged is None else jnp.where(lane == p, moved, merged)
                    out[tile * per_tile + d, i * GROUP : (i + 1) * GROUP, half * 128 : (half + 1) * 128] = merged.astype(out.dtype)


VMEM = pl.BlockSpec(memory_space=pltpu.VMEM)
SMEM = pl.BlockSpec(memory_space=pltpu.SMEM)
LIMIT = pltpu.CompilerParams(vmem_limit_bytes=24 * 1024 * 1024)


def placed(value):
    return pltpu.with_memory_space_constraint(value, pltpu.VMEM)


def resident(like):
    return pltpu.VMEM(like.shape, like.dtype)


def shards(record, pilot_sweep, sweep_table, owner_map):
    block_rows, channels = record.shape
    devices = lax.axis_size("tm")
    own = channels // devices
    blocks = SEG // BLOCK
    here = lax.axis_index("tm")
    width = block_rows + BLOCK
    kept = SEG - BLOCK
    back = [(k, k - 1) for k in range(1, devices)]
    forth = [(k, (k + 1) % devices) for k in range(devices)]
    first_rows = lax.ppermute(record[:kept, AHEAD:], "tm", back)
    last_rows = lax.ppermute(record[kept:SEG, AHEAD:], "tm", back)
    at = here.astype(jnp.int32).reshape(1)
    shape = jax.ShapeDtypeStruct
    pilot = jnp.pad(pilot_sweep.astype(F32), (0, width - pilot_sweep.shape[0]))[None]
    taps, taps_before, taps_last = pl.pallas_call(
        functools.partial(toeplitz_kernel, block_rows),
        out_shape=(shape((BLOCK, width), BF16), shape((BLOCK, SEG), BF16), resident(shape((BLOCK, BLOCK), BF16))),
        in_specs=[SMEM, SMEM, VMEM],
        out_specs=(VMEM,) * 3,
        name="toeplitz",
    )(at, sweep_table, pilot)
    piece = shape((blocks, BLOCK, AHEAD), F32)
    near, behind = pl.pallas_call(
        side_kernel,
        grid=(1,),
        out_shape=(piece, piece),
        in_specs=[
            pl.BlockSpec((BLOCK, width), lambda i: (0, 0)),
            pl.BlockSpec((BLOCK, SEG), lambda i: (0, 0)),
            pl.BlockSpec((block_rows, AHEAD), lambda i: (0, 0)),
        ],
        out_specs=(pl.BlockSpec((blocks, BLOCK, AHEAD), lambda i: (0, 0, 0)),) * 2,
        compiler_params=LIMIT,
        name="side",
    )(taps, taps_before, record)
    ahead = lax.ppermute(near, "tm", forth)
    others = channels - AHEAD
    near = pl.pallas_call(
        near_kernel,
        grid=(others // TILE,),
        out_shape=shape((blocks, BLOCK, others), F32),
        in_specs=[
            pl.BlockSpec((BLOCK, width), lambda i: (0, 0)),
            pl.BlockSpec((block_rows, TILE), lambda i: (0, i + AHEAD // TILE)),
        ],
        out_specs=pl.BlockSpec((blocks, BLOCK, TILE), lambda i: (0, 0, i)),
        compiler_params=LIMIT,
        name="near",
    )(taps, record)
    early, last = pl.pallas_call(
        far_kernel,
        out_shape=(resident(shape((others, kept), BF16)), resident(shape((BLOCK, others), F32))),
        in_specs=[SMEM] * 2 + [VMEM] * 3,
        out_specs=(VMEM,) * 2,
        compiler_params=LIMIT,
        name="far",
    )(at, sweep_table, *map(placed, (taps, near, first_rows)))
    traces = pl.pallas_call(
        late_kernel,
        out_shape=shape((channels, SEG), BF16),
        in_specs=[SMEM] * 2 + [VMEM] * 6,
        out_specs=VMEM,
        compiler_params=LIMIT,
        name="late",
    )(at, sweep_table, *map(placed, (taps_last, last, last_rows, ahead, behind, early)))
    samples = lax.all_to_all(traces.reshape(devices, own, SEG), "tm", 0, 0, tiled=True)

    groups = own // GROUP
    sweeps = sweep_table.shape[1]
    size = sweeps * GROUP
    wide = lax.axis_size("chan")
    square = shape((groups, sweeps, size), F32)
    side_shape = shape((groups, sweeps, 128), F32)
    row_shape = shape((groups, 1, size), F32)
    one = shape((wide, 1, 128), F32)
    scale = 1.0 / (devices * channels * wide)

    def exchanged(total):
        row = lax.all_to_all(total, "chan", 0, 0, tiled=True).sum(axis=0)
        return lax.all_to_all(jnp.broadcast_to(row[None], (devices, *row.shape)), "tm", 0, 0, tiled=True)

    tables = (row_shape, square, square, side_shape, row_shape, side_shape, row_shape)
    samples = placed(samples)
    keys, same, gram, norm_side, norm_row, side, row, total = pl.pallas_call(
        gram_kernel,
        out_shape=(*map(resident, tables), one),
        in_specs=[SMEM] * 3 + [VMEM],
        out_specs=(VMEM,) * (len(tables) + 1),
        compiler_params=LIMIT,
        name="gram",
    )(at, sweep_table, owner_map, samples)
    for _ in range(ITERS - 1):
        side, row, total = pl.pallas_call(
            functools.partial(update_kernel, scale),
            out_shape=(resident(side_shape), resident(row_shape), one),
            in_specs=[VMEM] * 7,
            out_specs=(VMEM,) * 3,
            compiler_params=LIMIT,
            name="update",
        )(placed(exchanged(total)), *map(placed, (same, gram, norm_side, norm_row, side, row)))
    shots = owner_map.shape[0]
    span = SEG // devices
    parts = pl.pallas_call(
        functools.partial(stack_kernel, scale, shots),
        out_shape=shape((devices, own, shots * span), BF16),
        in_specs=[VMEM] * 6,
        out_specs=VMEM,
        compiler_params=LIMIT,
        name="stack",
    )(placed(exchanged(total)), *map(placed, (samples, keys, same, side, row)))
    arrived = lax.all_to_all(parts, "tm", 0, 0, tiled=True)
    return arrived.reshape(channels, shots * span).T.astype(F32).reshape(shots, span, channels)


def solution(mesh):
    placed = (P("tm", "chan"), P(), P(), P())
    return jax.shard_map(
        shards, mesh=mesh, in_specs=placed, out_specs=P(None, "tm", "chan"), check_vma=False
    )
```

```python
import functools

import jax
import jax.numpy as jnp
from jax import lax
from jax.experimental import pallas as pl
from jax.experimental.pallas import tpu as pltpu
from jax.sharding import PartitionSpec as P

SEG = 1024
ITERS = 3
EPSILON = 1e-06
BLOCK = 256
GROUP = 8
STEP = 16
AHEAD = 512
TILE = 256
F32 = jnp.float32
F16 = jnp.float16
PEAK = 16384.0
TINY = 1e-30
BF16 = jnp.bfloat16


def shifted_rows(row, out):
    base = pltpu.roll(jnp.broadcast_to(row, (STEP, row.shape[1])), 0, 1, stride=1, stride_axis=0)
    skip = row.shape[1] - out.shape[1]
    for k in range(BLOCK // STEP):
        moved = base if k == 0 else pltpu.roll(base, STEP * k, 1)
        out[k * STEP : (k + 1) * STEP, :] = moved[:, skip:].astype(out.dtype)


def toeplitz_kernel(block_rows, here, table, pilot, taps, taps_before, taps_last):
    at = here[0]
    before = jnp.where(at == 0, table.shape[1] - 1, at - 1)
    skip = pilot.shape[1] - taps_before.shape[1] - BLOCK
    shifted_rows(pltpu.roll(pilot[...], table[0, at] - at * block_rows, 1), taps)
    moved = pltpu.roll(pilot[...], table[0, before] - before * block_rows, 1)[:, skip:]
    shifted_rows(jnp.where(at == 0, 0.0, moved), taps_before)
    taps_last[...] = taps[:, block_rows:]


def sign_of(table, column):
    return 1.0 - 2.0 * (table[2, column] % 2).astype(F32)


def transposed_into(out, first, block, values, sign):
    rounded = (values * sign).astype(BF16)
    for k in range(values.shape[1] // 128):
        out[first + 128 * k : first + 128 * (k + 1), block * BLOCK : (block + 1) * BLOCK] = rounded[:, 128 * k : 128 * (k + 1)].T


def side_kernel(taps, record, near_out, peak_out):
    rows = record.shape[0]
    peak = jnp.zeros((1, 1), F32)
    for b in range(near_out.shape[0]):
        product = jnp.dot(taps[:, : rows - BLOCK * b], record[BLOCK * b :, :], preferred_element_type=F32)
        near_out[b] = product
        peak = jnp.maximum(peak, jnp.max(jnp.abs(product), keepdims=True))
    peak = jnp.maximum(peak, TINY)
    for b in range(near_out.shape[0]):
        near_out[b] = near_out[b] * (PEAK / peak)
    peak_out[...] = jnp.broadcast_to(peak * (1.0 / PEAK), peak_out.shape)


def behind_kernel(taps_before, record, behind_out):
    for b in range(behind_out.shape[0]):
        kept = taps_before.shape[1] - BLOCK * (b + 1)
        behind_out[b] = jnp.dot(taps_before[:, kept:], record[: BLOCK * (b + 1), :], preferred_element_type=F32)


def near_kernel(taps, record, near_out):
    rows = record.shape[0]
    for b in range(near_out.shape[0]):
        product = jnp.dot(taps[:, : rows - BLOCK * b], record[BLOCK * b :, :], preferred_element_type=F32)
        near_out[b] = product


def far_kernel(here, table, taps, near, following, early_out, last_out):
    sign = sign_of(table, here[0])
    count = near.shape[0]
    for t in range(near.shape[2] // TILE):
        part = slice(TILE * t, TILE * (t + 1))
        for b in range(count):
            rows = min(BLOCK * (b + 1), following.shape[0])
            split = taps.shape[1] - BLOCK * (b + 1)
            product = jnp.dot(taps[:, split : split + rows], following[:rows, part], preferred_element_type=F32)
            values = near[b, :, part] + product
            if b < count - 1:
                transposed_into(early_out, TILE * t, b, values, sign)
            else:
                last_out[:, part] = values


def late_kernel(here, table, taps_last, last, rest, early, *refs):
    *pieces, out = refs
    at = here[0]
    before = jnp.where(at == 0, table.shape[1] - 1, at - 1)
    count = pieces[0].shape[0]
    out[AHEAD:, : early.shape[1]] = early[...]
    for t, piece in enumerate(pieces):
        for b in range(count):
            transposed_into(out, TILE * t, b, piece[b].astype(F32), sign_of(table, before))
    product = jnp.dot(taps_last[...], rest[...], preferred_element_type=F32)
    transposed_into(out, AHEAD, count - 1, last[...] + product, sign_of(table, at))


def lane_sum(values):
    row = values[:, :128] + values[:, 128:]
    step = GROUP
    while step < 128:
        row = row + pltpu.roll(row, step, 1)
        step *= 2
    return row


def twice(values):
    return jnp.concatenate([values, values], axis=1)


def down(values):
    return jnp.sum(values, axis=0, keepdims=True)


def combined(norm, cross, total, square):
    inverse = 1.0 / total
    energy = norm - 2.0 * cross * inverse + square * inverse * inverse
    return jnp.maximum(energy, 0.0) * (1.0 / SEG)


def residual_energy(gram, same, norm_side, norm_row, side, row):
    wide = twice(side)
    cross_side = lane_sum(gram * row)
    cross_row = down(gram * wide)
    total_side = lane_sum(same * row)
    total_row = down(same * wide)
    square_side = lane_sum(same * (row * cross_row))
    square_row = down(same * twice(side * cross_side))
    return combined(norm_side, cross_side, total_side, square_side), combined(norm_row, cross_row, total_row, square_row)


def group_rows(samples, i):
    part = samples[:, i * GROUP : (i + 1) * GROUP, :].astype(F32)
    return part.reshape(part.shape[0] * GROUP, part.shape[2]).astype(BF16)


def gram_kernel(here, table, owner, samples, keys, same_out, gram_out, norm_side, norm_row, energy_side, energy_row, total_out):
    groups = gram_out.shape[0]
    sweeps = table.shape[1]
    size = sweeps * GROUP
    lane = lax.broadcasted_iota(jnp.int32, (1, size), 1)
    line = lax.broadcasted_iota(jnp.int32, (sweeps, 1), 0)
    usual_row = moved_row = jnp.zeros((1, size), jnp.int32)
    usual_side = moved_side = jnp.zeros((sweeps, 1), jnp.int32)
    for g in range(sweeps):
        slot = owner[table[1, g]]
        after = (g + 1) % sweeps
        usual_row = jnp.where(lane // GROUP == g, slot, usual_row)
        usual_side = jnp.where(line == g, slot, usual_side)
        moved_row = jnp.where(lane // GROUP == after, slot, moved_row)
        moved_side = jnp.where(line == after, slot, moved_side)
    matching = lax.broadcasted_iota(jnp.int32, (GROUP, size), 0) == lane % GROUP
    ones = jnp.ones((sweeps, 128), F32)
    total = jnp.zeros((1, size), F32)
    for i in range(groups):
        ahead = (here[0] * groups + i) * GROUP < AHEAD
        row = jnp.where(ahead, moved_row, usual_row)
        side = jnp.where(ahead, moved_side, usual_side)
        keys[i] = (row * GROUP + lane % GROUP).astype(F32)
        same = (side == row).astype(F32)
        rows = group_rows(samples, i)
        product = lax.dot_general(rows, rows, (((1,), (1,)), ((), ())), preferred_element_type=F32)
        parts = product.reshape(sweeps, GROUP, size)
        full = jnp.sum(jnp.where(matching[None], parts, 0.0), axis=1)
        own = jnp.where(line == lane // GROUP, full, 0.0)
        gram = full * same
        norms = (lane_sum(own), down(own))
        same_out[i] = same
        gram_out[i] = gram
        norm_side[i], norm_row[i] = norms
        energy_side[i], energy = residual_energy(gram, same, *norms, ones, jnp.ones((1, size), F32))
        energy_row[i] = energy
        total = total + energy
    total_out[...] = jnp.broadcast_to(jnp.sum(total, axis=1, keepdims=True), total_out.shape)


def spread_of(arrived, scale):
    return jnp.sum(arrived[...], axis=0)[:, :1] * scale + EPSILON


def update_kernel(scale, arrived, same, gram, norm_side, norm_row, side_in, row_in, energy_side, energy_row, total_out):
    spread = spread_of(arrived, scale)
    total = jnp.zeros(row_in.shape[1:], F32)
    for i in range(gram.shape[0]):
        side = 1.0 / (1.0 + side_in[i] / spread)
        row = 1.0 / (1.0 + row_in[i] / spread)
        energy_side[i], energy = residual_energy(gram[i], same[i], norm_side[i], norm_row[i], side, row)
        energy_row[i] = energy
        total = total + energy
    total_out[...] = jnp.broadcast_to(jnp.sum(total, axis=1, keepdims=True), total_out.shape)


def stack_kernel(scale, shots, arrived, samples, keys, same, side_in, row_in, out):
    spread = spread_of(arrived, scale)
    size = keys.shape[2]
    slots = lax.broadcasted_iota(jnp.int32, (shots * GROUP, size), 0).astype(F32)
    span = out.shape[2] // shots
    per_tile = 128 // span
    lane = lax.broadcasted_iota(jnp.int32, (GROUP, 128), 1) // span
    for i in range(keys.shape[0]):
        rows = group_rows(samples, i)
        side = 1.0 / (1.0 + side_in[i] / spread)
        row = 1.0 / (1.0 + row_in[i] / spread)
        factor = jnp.where(slots == keys[i], row / down(same[i] * twice(side)), 0.0)
        high = factor.astype(BF16)
        rest = factor - high.astype(F32)
        middle = rest.astype(BF16)
        low = (rest - middle.astype(F32)).astype(BF16)
        products = jnp.dot(jnp.concatenate([high, middle, low], axis=0), rows, preferred_element_type=F32)
        count = shots * GROUP
        stack = products[:count] + products[count : 2 * count] + products[2 * count :]
        for tile in range(stack.shape[1] // 128):
            for half in range(shots // per_tile):
                pieces = []
                for p in range(per_tile):
                    k = half * per_tile + p
                    pieces.append(stack[k * GROUP : (k + 1) * GROUP, tile * 128 : (tile + 1) * 128])
                for d in range(per_tile):
                    merged = None
                    for p in range(per_tile):
                        moved = pieces[p] if p == d else pltpu.roll(pieces[p], (span * (p - d)) % 128, 1)
                        merged = moved if merged is None else jnp.where(lane == p, moved, merged)
                    out[tile * per_tile + d, i * GROUP : (i + 1) * GROUP, half * 128 : (half + 1) * 128] = merged.astype(out.dtype)


VMEM = pl.BlockSpec(memory_space=pltpu.VMEM)
SMEM = pl.BlockSpec(memory_space=pltpu.SMEM)
LIMIT = pltpu.CompilerParams(vmem_limit_bytes=24 * 1024 * 1024)


def placed(value):
    return pltpu.with_memory_space_constraint(value, pltpu.VMEM)


def resident(like):
    return pltpu.VMEM(like.shape, like.dtype)


def shards(record, pilot_sweep, sweep_table, owner_map):
    block_rows, channels = record.shape
    devices = lax.axis_size("tm")
    own = channels // devices
    blocks = SEG // BLOCK
    here = lax.axis_index("tm")
    width = block_rows + BLOCK
    kept = SEG - BLOCK
    back = [(k, k - 1) for k in range(1, devices)]
    forth = [(k, (k + 1) % devices) for k in range(devices)]
    first_rows = lax.ppermute(record[:kept, AHEAD:], "tm", back)
    last_rows = lax.ppermute(record[kept:SEG, AHEAD:], "tm", back)
    at = here.astype(jnp.int32).reshape(1)
    shape = jax.ShapeDtypeStruct
    pilot = jnp.pad(pilot_sweep.astype(F32), (0, width - pilot_sweep.shape[0]))[None]
    taps, taps_before, taps_last = pl.pallas_call(
        functools.partial(toeplitz_kernel, block_rows),
        out_shape=(shape((BLOCK, width), BF16), shape((BLOCK, SEG), BF16), resident(shape((BLOCK, BLOCK), BF16))),
        in_specs=[SMEM, SMEM, VMEM],
        out_specs=(VMEM,) * 3,
        name="toeplitz",
    )(at, sweep_table, pilot)
    sent, peaks = [], []
    for t in range(AHEAD // TILE):
        near, peak = pl.pallas_call(
            side_kernel,
            grid=(1,),
            out_shape=(shape((blocks, BLOCK, TILE), F32), shape((8, 128), F32)),
            in_specs=[pl.BlockSpec((BLOCK, width), lambda i: (0, 0)), pl.BlockSpec((block_rows, TILE), lambda i, t=t: (0, t))],
            out_specs=(pl.BlockSpec((blocks, BLOCK, TILE), lambda i: (0, 0, 0)), pl.BlockSpec((8, 128), lambda i: (0, 0))),
            compiler_params=LIMIT,
            name="side",
        )(taps, record)
        sent.append(lax.ppermute(near.astype(F16), "tm", forth))
        peaks.append(peak)
    peaks = lax.ppermute(jnp.stack(peaks), "tm", forth)
    behind = pl.pallas_call(
        behind_kernel,
        grid=(AHEAD // TILE,),
        out_shape=shape((blocks, BLOCK, AHEAD), F32),
        in_specs=[pl.BlockSpec((BLOCK, SEG), lambda i: (0, 0)), pl.BlockSpec((SEG, TILE), lambda i: (0, i))],
        out_specs=pl.BlockSpec((blocks, BLOCK, TILE), lambda i: (0, 0, i)),
        compiler_params=LIMIT,
        name="behind",
    )(taps_before, record)
    pieces = []
    for t, scaled in enumerate(sent):
        ahead = scaled.astype(F32) * peaks[t, :1, :1]
        pieces.append((ahead + behind[:, :, TILE * t : TILE * (t + 1)]).astype(BF16))
    others = channels - AHEAD
    near = pl.pallas_call(
        near_kernel,
        grid=(others // TILE,),
        out_shape=shape((blocks, BLOCK, others), F32),
        in_specs=[
            pl.BlockSpec((BLOCK, width), lambda i: (0, 0)),
            pl.BlockSpec((block_rows, TILE), lambda i: (0, i + AHEAD // TILE)),
        ],
        out_specs=pl.BlockSpec((blocks, BLOCK, TILE), lambda i: (0, 0, i)),
        compiler_params=LIMIT,
        name="near",
    )(taps, record)
    early, last = pl.pallas_call(
        far_kernel,
        out_shape=(resident(shape((others, kept), BF16)), resident(shape((BLOCK, others), F32))),
        in_specs=[SMEM] * 2 + [VMEM] * 3,
        out_specs=(VMEM,) * 2,
        compiler_params=LIMIT,
        name="far",
    )(at, sweep_table, *map(placed, (taps, near, first_rows)))
    traces = pl.pallas_call(
        late_kernel,
        out_shape=shape((channels, SEG), BF16),
        in_specs=[SMEM] * 2 + [VMEM] * (4 + len(pieces)),
        out_specs=VMEM,
        compiler_params=LIMIT,
        name="late",
    )(at, sweep_table, *map(placed, (taps_last, last, last_rows, early, *pieces)))
    samples = lax.all_to_all(traces.reshape(devices, own, SEG), "tm", 0, 0, tiled=True)

    groups = own // GROUP
    sweeps = sweep_table.shape[1]
    size = sweeps * GROUP
    wide = lax.axis_size("chan")
    square = shape((groups, sweeps, size), F32)
    side_shape = shape((groups, sweeps, 128), F32)
    row_shape = shape((groups, 1, size), F32)
    one = shape((wide, 1, 128), F32)
    scale = 1.0 / (devices * channels * wide)

    def exchanged(total):
        row = lax.all_to_all(total, "chan", 0, 0, tiled=True).sum(axis=0)
        return lax.all_to_all(jnp.broadcast_to(row[None], (devices, *row.shape)), "tm", 0, 0, tiled=True)

    tables = (row_shape, square, square, side_shape, row_shape, side_shape, row_shape)
    samples = placed(samples)
    keys, same, gram, norm_side, norm_row, side, row, total = pl.pallas_call(
        gram_kernel,
        out_shape=(*map(resident, tables), one),
        in_specs=[SMEM] * 3 + [VMEM],
        out_specs=(VMEM,) * (len(tables) + 1),
        compiler_params=LIMIT,
        name="gram",
    )(at, sweep_table, owner_map, samples)
    for _ in range(ITERS - 1):
        side, row, total = pl.pallas_call(
            functools.partial(update_kernel, scale),
            out_shape=(resident(side_shape), resident(row_shape), one),
            in_specs=[VMEM] * 7,
            out_specs=(VMEM,) * 3,
            compiler_params=LIMIT,
            name="update",
        )(placed(exchanged(total)), *map(placed, (same, gram, norm_side, norm_row, side, row)))
    shots = owner_map.shape[0]
    span = SEG // devices
    parts = pl.pallas_call(
        functools.partial(stack_kernel, scale, shots),
        out_shape=shape((devices, own, shots * span), BF16),
        in_specs=[VMEM] * 6,
        out_specs=VMEM,
        compiler_params=LIMIT,
        name="stack",
    )(placed(exchanged(total)), *map(placed, (samples, keys, same, side, row)))
    arrived = lax.all_to_all(parts, "tm", 0, 0, tiled=True)
    return arrived.reshape(channels, shots * span).T.astype(F32).reshape(shots, span, channels)


def solution(mesh):
    placed = (P("tm", "chan"), P(), P(), P())
    return jax.shard_map(
        shards, mesh=mesh, in_specs=placed, out_specs=P(None, "tm", "chan"), check_vma=False
    )
```

```python
import functools

import jax
import jax.numpy as jnp
from jax import lax
from jax.experimental import pallas as pl
from jax.experimental.pallas import tpu as pltpu
from jax.sharding import PartitionSpec as P

SEG = 1024
ITERS = 3
EPSILON = 1e-06
BLOCK = 256
GROUP = 8
STEP = 16
AHEAD = 512
TILE = 256
F32 = jnp.float32
F16 = jnp.float16
PEAK = 16384.0
TINY = 1e-30
BF16 = jnp.bfloat16


def shifted_rows(row, out):
    base = pltpu.roll(jnp.broadcast_to(row, (STEP, row.shape[1])), 0, 1, stride=1, stride_axis=0)
    skip = row.shape[1] - out.shape[1]
    for k in range(BLOCK // STEP):
        moved = base if k == 0 else pltpu.roll(base, STEP * k, 1)
        out[k * STEP : (k + 1) * STEP, :] = moved[:, skip:].astype(out.dtype)


def toeplitz_kernel(block_rows, here, table, pilot, taps, taps_before, taps_last):
    at = here[0]
    before = jnp.where(at == 0, table.shape[1] - 1, at - 1)
    skip = pilot.shape[1] - taps_before.shape[1] - BLOCK
    shifted_rows(pltpu.roll(pilot[...], table[0, at] - at * block_rows, 1), taps)
    moved = pltpu.roll(pilot[...], table[0, before] - before * block_rows, 1)[:, skip:]
    shifted_rows(jnp.where(at == 0, 0.0, moved), taps_before)
    taps_last[...] = taps[:, block_rows:]


def sign_of(table, column):
    return 1.0 - 2.0 * (table[2, column] % 2).astype(F32)


def transposed_into(out, first, block, values, sign):
    rounded = (values * sign).astype(BF16)
    for k in range(values.shape[1] // 128):
        out[first + 128 * k : first + 128 * (k + 1), block * BLOCK : (block + 1) * BLOCK] = rounded[:, 128 * k : 128 * (k + 1)].T


def side_kernel(taps, record, near_out, peak_out):
    rows = record.shape[0]
    peak = jnp.zeros((1, 1), F32)
    for b in range(near_out.shape[0]):
        product = jnp.dot(taps[:, : rows - BLOCK * b], record[BLOCK * b :, :], preferred_element_type=F32)
        near_out[b] = product
        peak = jnp.maximum(peak, jnp.max(jnp.abs(product), keepdims=True))
    peak = jnp.maximum(peak, TINY)
    for b in range(near_out.shape[0]):
        near_out[b] = near_out[b] * (PEAK / peak)
    peak_out[...] = jnp.broadcast_to(peak * (1.0 / PEAK), peak_out.shape)


def behind_kernel(taps_before, record, behind_out):
    for b in range(behind_out.shape[0]):
        kept = taps_before.shape[1] - BLOCK * (b + 1)
        behind_out[b] = jnp.dot(taps_before[:, kept:], record[: BLOCK * (b + 1), :], preferred_element_type=F32)


def near_kernel(taps, record, near_out):
    rows = record.shape[0]
    for b in range(near_out.shape[0]):
        product = jnp.dot(taps[:, : rows - BLOCK * b], record[BLOCK * b :, :], preferred_element_type=F32)
        near_out[b] = product


def far_kernel(here, table, taps, near, following, early_out, last_out):
    sign = sign_of(table, here[0])
    count = near.shape[0]
    for t in range(near.shape[2] // TILE):
        part = slice(TILE * t, TILE * (t + 1))
        for b in range(count):
            rows = min(BLOCK * (b + 1), following.shape[0])
            split = taps.shape[1] - BLOCK * (b + 1)
            product = jnp.dot(taps[:, split : split + rows], following[:rows, part], preferred_element_type=F32)
            values = near[b, :, part] + product
            if b < count - 1:
                transposed_into(early_out, TILE * t, b, values, sign)
            else:
                last_out[:, part] = values


def late_kernel(here, table, taps_last, last, rest, early, *refs):
    *pieces, out = refs
    at = here[0]
    before = jnp.where(at == 0, table.shape[1] - 1, at - 1)
    count = pieces[0].shape[0]
    out[AHEAD:, : early.shape[1]] = early[...]
    for t, piece in enumerate(pieces):
        for b in range(count):
            transposed_into(out, TILE * t, b, piece[b].astype(F32), sign_of(table, before))
    product = jnp.dot(taps_last[...], rest[...], preferred_element_type=F32)
    transposed_into(out, AHEAD, count - 1, last[...] + product, sign_of(table, at))


def lane_sum(values):
    row = values[:, :128] + values[:, 128:]
    step = GROUP
    while step < 128:
        row = row + pltpu.roll(row, step, 1)
        step *= 2
    return row


def twice(values):
    return jnp.concatenate([values, values], axis=1)


def down(values):
    return jnp.sum(values, axis=0, keepdims=True)


def combined(norm, cross, total, square):
    inverse = 1.0 / total
    energy = norm - 2.0 * cross * inverse + square * inverse * inverse
    return jnp.maximum(energy, 0.0) * (1.0 / SEG)


def residual_energy(gram, same, norm_side, norm_row, side, row):
    wide = twice(side)
    cross_side = lane_sum(gram * row)
    cross_row = down(gram * wide)
    total_side = lane_sum(same * row)
    total_row = down(same * wide)
    square_side = lane_sum(same * (row * cross_row))
    square_row = down(same * twice(side * cross_side))
    return combined(norm_side, cross_side, total_side, square_side), combined(norm_row, cross_row, total_row, square_row)


def group_rows(samples, i):
    part = samples[:, i * GROUP : (i + 1) * GROUP, :].astype(F32)
    return part.reshape(part.shape[0] * GROUP, part.shape[2]).astype(BF16)


def gram_kernel(here, table, owner, samples, keys, same_out, gram_out, norm_side, norm_row, energy_side, energy_row, total_out):
    groups = gram_out.shape[0]
    sweeps = table.shape[1]
    size = sweeps * GROUP
    lane = lax.broadcasted_iota(jnp.int32, (1, size), 1)
    line = lax.broadcasted_iota(jnp.int32, (sweeps, 1), 0)
    usual_row = moved_row = jnp.zeros((1, size), jnp.int32)
    usual_side = moved_side = jnp.zeros((sweeps, 1), jnp.int32)
    for g in range(sweeps):
        slot = owner[table[1, g]]
        after = (g + 1) % sweeps
        usual_row = jnp.where(lane // GROUP == g, slot, usual_row)
        usual_side = jnp.where(line == g, slot, usual_side)
        moved_row = jnp.where(lane // GROUP == after, slot, moved_row)
        moved_side = jnp.where(line == after, slot, moved_side)
    matching = lax.broadcasted_iota(jnp.int32, (GROUP, size), 0) == lane % GROUP
    ones = jnp.ones((sweeps, 128), F32)
    total = jnp.zeros((1, size), F32)
    for i in range(groups):
        ahead = (here[0] * groups + i) * GROUP < AHEAD
        row = jnp.where(ahead, moved_row, usual_row)
        side = jnp.where(ahead, moved_side, usual_side)
        keys[i] = (row * GROUP + lane % GROUP).astype(F32)
        same = (side == row).astype(F32)
        rows = group_rows(samples, i)
        product = lax.dot_general(rows, rows, (((1,), (1,)), ((), ())), preferred_element_type=F32)
        parts = product.reshape(sweeps, GROUP, size)
        full = jnp.sum(jnp.where(matching[None], parts, 0.0), axis=1)
        own = jnp.where(line == lane // GROUP, full, 0.0)
        gram = full * same
        norms = (lane_sum(own), down(own))
        same_out[i] = same
        gram_out[i] = gram
        norm_side[i], norm_row[i] = norms
        energy_side[i], energy = residual_energy(gram, same, *norms, ones, jnp.ones((1, size), F32))
        energy_row[i] = energy
        total = total + energy
    total_out[...] = jnp.broadcast_to(jnp.sum(total, axis=1, keepdims=True), total_out.shape)


def spread_of(arrived, scale):
    return jnp.sum(arrived[...], axis=0)[:, :1] * scale + EPSILON


def update_kernel(scale, arrived, same, gram, norm_side, norm_row, side_in, row_in, energy_side, energy_row, total_out):
    spread = spread_of(arrived, scale)
    total = jnp.zeros(row_in.shape[1:], F32)
    for i in range(gram.shape[0]):
        side = 1.0 / (1.0 + side_in[i] / spread)
        row = 1.0 / (1.0 + row_in[i] / spread)
        energy_side[i], energy = residual_energy(gram[i], same[i], norm_side[i], norm_row[i], side, row)
        energy_row[i] = energy
        total = total + energy
    total_out[...] = jnp.broadcast_to(jnp.sum(total, axis=1, keepdims=True), total_out.shape)


def stack_kernel(scale, shots, arrived, samples, keys, same, side_in, row_in, out):
    spread = spread_of(arrived, scale)
    size = keys.shape[2]
    slots = lax.broadcasted_iota(jnp.int32, (shots * GROUP, size), 0).astype(F32)
    span = out.shape[2] // shots
    per_tile = 128 // span
    lane = lax.broadcasted_iota(jnp.int32, (GROUP, 128), 1) // span
    for i in range(keys.shape[0]):
        rows = group_rows(samples, i)
        side = 1.0 / (1.0 + side_in[i] / spread)
        row = 1.0 / (1.0 + row_in[i] / spread)
        factor = jnp.where(slots == keys[i], row / down(same[i] * twice(side)), 0.0)
        high = factor.astype(BF16)
        rest = factor - high.astype(F32)
        middle = rest.astype(BF16)
        low = (rest - middle.astype(F32)).astype(BF16)
        products = jnp.dot(jnp.concatenate([high, middle, low], axis=0), rows, preferred_element_type=F32)
        count = shots * GROUP
        stack = products[:count] + products[count : 2 * count] + products[2 * count :]
        for tile in range(stack.shape[1] // 128):
            for half in range(shots // per_tile):
                pieces = []
                for p in range(per_tile):
                    k = half * per_tile + p
                    pieces.append(stack[k * GROUP : (k + 1) * GROUP, tile * 128 : (tile + 1) * 128])
                for d in range(per_tile):
                    merged = None
                    for p in range(per_tile):
                        moved = pieces[p] if p == d else pltpu.roll(pieces[p], (span * (p - d)) % 128, 1)
                        merged = moved if merged is None else jnp.where(lane == p, moved, merged)
                    out[tile * per_tile + d, i * GROUP : (i + 1) * GROUP, half * 128 : (half + 1) * 128] = merged.astype(out.dtype)


VMEM = pl.BlockSpec(memory_space=pltpu.VMEM)
SMEM = pl.BlockSpec(memory_space=pltpu.SMEM)
LIMIT = pltpu.CompilerParams(vmem_limit_bytes=24 * 1024 * 1024)


def placed(value):
    return pltpu.with_memory_space_constraint(value, pltpu.VMEM)


def resident(like):
    return pltpu.VMEM(like.shape, like.dtype)


def shards(record, pilot_sweep, sweep_table, owner_map):
    block_rows, channels = record.shape
    devices = lax.axis_size("tm")
    own = channels // devices
    blocks = SEG // BLOCK
    here = lax.axis_index("tm")
    width = block_rows + BLOCK
    kept = SEG - BLOCK
    back = [(k, k - 1) for k in range(1, devices)]
    forth = [(k, (k + 1) % devices) for k in range(devices)]
    first_rows = lax.ppermute(record[:kept, AHEAD:], "tm", back)
    last_rows = lax.ppermute(record[kept:SEG, AHEAD:], "tm", back)
    at = here.astype(jnp.int32).reshape(1)
    shape = jax.ShapeDtypeStruct
    pilot = jnp.pad(pilot_sweep.astype(F32), (0, width - pilot_sweep.shape[0]))[None]
    taps, taps_before, taps_last = pl.pallas_call(
        functools.partial(toeplitz_kernel, block_rows),
        out_shape=tuple(resident(shape((BLOCK, n), BF16)) for n in (width, SEG, BLOCK)),
        in_specs=[SMEM, SMEM, VMEM],
        out_specs=(VMEM,) * 3,
        compiler_params=LIMIT,
        name="toeplitz",
    )(at, sweep_table, pilot)
    stored = pltpu.with_memory_space_constraint(record, pltpu.HBM)
    sent, peaks = [], []
    for t in range(AHEAD // TILE):
        near, peak = pl.pallas_call(
            side_kernel,
            grid=(1,),
            out_shape=(shape((blocks, BLOCK, TILE), F32), shape((8, 128), F32)),
            in_specs=[VMEM, pl.BlockSpec((block_rows, TILE), lambda i, t=t: (0, t))],
            out_specs=(pl.BlockSpec((blocks, BLOCK, TILE), lambda i: (0, 0, 0)), pl.BlockSpec((8, 128), lambda i: (0, 0))),
            compiler_params=LIMIT,
            name="side",
        )(placed(taps), stored)
        sent.append(lax.ppermute(near.astype(F16), "tm", forth))
        peaks.append(peak)
    peaks = lax.ppermute(jnp.stack(peaks), "tm", forth)
    behind = pl.pallas_call(
        behind_kernel,
        grid=(AHEAD // TILE,),
        out_shape=shape((blocks, BLOCK, AHEAD), F32),
        in_specs=[VMEM, pl.BlockSpec((SEG, TILE), lambda i: (0, i))],
        out_specs=pl.BlockSpec((blocks, BLOCK, TILE), lambda i: (0, 0, i)),
        compiler_params=LIMIT,
        name="behind",
    )(placed(taps_before), stored)
    others = channels - AHEAD
    near = pl.pallas_call(
        near_kernel,
        grid=(others // TILE,),
        out_shape=shape((blocks, BLOCK, others), F32),
        in_specs=[
            VMEM,
            pl.BlockSpec((block_rows, TILE), lambda i: (0, i + AHEAD // TILE)),
        ],
        out_specs=pl.BlockSpec((blocks, BLOCK, TILE), lambda i: (0, 0, i)),
        compiler_params=LIMIT,
        name="near",
    )(placed(taps), stored)
    early, last = pl.pallas_call(
        far_kernel,
        out_shape=(resident(shape((others, kept), BF16)), resident(shape((BLOCK, others), F32))),
        in_specs=[SMEM] * 2 + [VMEM] * 3,
        out_specs=(VMEM,) * 2,
        compiler_params=LIMIT,
        name="far",
    )(at, sweep_table, *map(placed, (taps, near, first_rows)))
    early, last, peaks, *sent = lax.optimization_barrier((early, last, peaks, *sent))
    pieces = []
    for t, scaled in enumerate(sent):
        ahead = scaled.astype(F32) * peaks[t, :1, :1]
        pieces.append((ahead + behind[:, :, TILE * t : TILE * (t + 1)]).astype(BF16))
    traces = pl.pallas_call(
        late_kernel,
        out_shape=shape((channels, SEG), BF16),
        in_specs=[SMEM] * 2 + [VMEM] * (4 + len(pieces)),
        out_specs=VMEM,
        compiler_params=LIMIT,
        name="late",
    )(at, sweep_table, *map(placed, (taps_last, last, last_rows, early, *pieces)))
    samples = lax.all_to_all(traces.reshape(devices, own, SEG), "tm", 0, 0, tiled=True)

    groups = own // GROUP
    sweeps = sweep_table.shape[1]
    size = sweeps * GROUP
    wide = lax.axis_size("chan")
    square = shape((groups, sweeps, size), F32)
    side_shape = shape((groups, sweeps, 128), F32)
    row_shape = shape((groups, 1, size), F32)
    one = shape((wide, 1, 128), F32)
    scale = 1.0 / (devices * channels * wide)

    def exchanged(total):
        row = lax.all_to_all(total, "chan", 0, 0, tiled=True).sum(axis=0)
        return lax.all_to_all(jnp.broadcast_to(row[None], (devices, *row.shape)), "tm", 0, 0, tiled=True)

    tables = (row_shape, square, square, side_shape, row_shape, side_shape, row_shape)
    samples = placed(samples)
    keys, same, gram, norm_side, norm_row, side, row, total = pl.pallas_call(
        gram_kernel,
        out_shape=(*map(resident, tables), one),
        in_specs=[SMEM] * 3 + [VMEM],
        out_specs=(VMEM,) * (len(tables) + 1),
        compiler_params=LIMIT,
        name="gram",
    )(at, sweep_table, owner_map, samples)
    for _ in range(ITERS - 1):
        side, row, total = pl.pallas_call(
            functools.partial(update_kernel, scale),
            out_shape=(resident(side_shape), resident(row_shape), one),
            in_specs=[VMEM] * 7,
            out_specs=(VMEM,) * 3,
            compiler_params=LIMIT,
            name="update",
        )(placed(exchanged(total)), *map(placed, (same, gram, norm_side, norm_row, side, row)))
    shots = owner_map.shape[0]
    span = SEG // devices
    parts = pl.pallas_call(
        functools.partial(stack_kernel, scale, shots),
        out_shape=shape((devices, own, shots * span), BF16),
        in_specs=[VMEM] * 6,
        out_specs=VMEM,
        compiler_params=LIMIT,
        name="stack",
    )(placed(exchanged(total)), *map(placed, (samples, keys, same, side, row)))
    arrived = lax.all_to_all(parts, "tm", 0, 0, tiled=True)
    return arrived.reshape(channels, shots * span).T.astype(F32).reshape(shots, span, channels)


def solution(mesh):
    placed = (P("tm", "chan"), P(), P(), P())
    return jax.shard_map(
        shards, mesh=mesh, in_specs=placed, out_specs=P(None, "tm", "chan"), check_vma=False
    )
```
